32 devices in a mesh: slab: 4 (over z), tile: 8 (over y, x, core).
Axes of the slice: x: 2, y: 2, z: 4, core: 2. Of those that a mesh axis runs over, the one named last changes fastest.
Arguments:
- voxel_grid: float32 [4, 64, 64, 256], P(None, 'slab', 'tile'), may hold values from -4 to 4
- first_moment: float32 [4, 64, 64, 256], P(None, 'slab', 'tile'), may hold values from -0.75 to 0.75
- second_moment: float32 [4, 64, 64, 256], P(None, 'slab', 'tile'), may hold values from 0.01 to 0.5
- pixel_index: int32 [32768], P('tile'), may hold values from 0 to 2047
- start_slab: int32 [32768], P('tile'), may hold values from 0 to 1
- ray_count: int32 [32768], P('tile'), may hold values from 16 to 48
- target: float32 [3, 32768], P(None, 'tile'), may hold values from 0 to 1
Outputs:
- new_grid: float32 [4, 64, 64, 256], P(None, 'slab', 'tile')
- new_first: float32 [4, 64, 64, 256], P(None, 'slab', 'tile')
- new_second: float32 [4, 64, 64, 256], P(None, 'slab', 'tile')
The draws below stay inside these ranges and needn't reach their ends.
All inputs are finite; a program needn't handle non-finite values.
Results may differ from the reference program's by a relative error of at most 0.0003.
Values sent between devices are 32-bit elements; how exact they have to be, the bound alone decides.
A program may use at most 128 MiB of HBM per device.

```python
import math
import jax
import jax.numpy as jnp
from jax import lax

CZ = 16
CX = 8
NY = 256
RAYS_DEV = 4096
STEP = 20
NZ = 64
NX = 64
RAYS = 32768
HALF_SLABS = 2
N_TILE = 8


def place_ends(result, rng, least, top_value):
    longest = result.shape.index(max(result.shape))
    spots = []
    for shift in (0, 1):
        where = [jax.random.randint(jax.random.fold_in(rng, axis), (), 0, length) for axis, length in enumerate(result.shape)]
        where[longest] = (where[longest] + shift) % result.shape[longest]
        spots.append(tuple(where))
    return result.at[spots[0]].set(least).at[spots[1]].set(top_value)


def block_levels(key, shape, pieces, least, top_value):
    loudness = 1.0
    for axis_at, blocks in pieces:
        draws = jax.random.uniform(jax.random.fold_in(jax.random.fold_in(key, 6), axis_at), (blocks,), jnp.float32, least / len(pieces), top_value / len(pieces))
        loudness = loudness * jnp.repeat(jnp.exp(draws), shape[axis_at] // blocks).reshape((-1,) + (1,) * (len(shape) - 1 - axis_at))
    return loudness


def bell_draw(key, dims, spread, reach, split=(), kind=jnp.bfloat16):
    array = spread * jax.random.normal(key, dims, jnp.float32)
    if split:
        array = array * block_levels(key, dims, split, -0.22, 0.18)
    return jnp.clip(array, -reach, reach).astype(kind)


def setup_inputs(seed: int = 0) -> dict:
    seeds = jax.random.split(jax.random.key(seed), 8)
    return {
        "voxel_grid": bell_draw(seeds[0], (4, NZ, NX, NY), 1.0, 4.0, ((1, 4), (2, 8)), jnp.float32),
        "first_moment": bell_draw(seeds[1], (4, NZ, NX, NY), 0.05, 0.75, ((1, 4), (2, 8)), jnp.float32),
        "second_moment": jnp.clip(jnp.exp(math.log(0.5) - 3.912023 * jax.random.uniform(seeds[2], (4, NZ, NX, NY), jnp.float32) ** block_levels(seeds[2], (4, NZ, NX, NY), ((1, 4), (2, 8)), -0.2, 0.2)), 0.01, 0.5),
        "pixel_index": place_ends(jax.random.randint(seeds[3], (RAYS,), 0, CX * NY), jax.random.fold_in(seeds[3], 1), 0, (CX * NY) - 1).astype(jnp.int32),
        "start_slab": place_ends(jax.random.randint(seeds[4], (RAYS,), 0, HALF_SLABS), jax.random.fold_in(seeds[4], 1), 0, HALF_SLABS - 1).astype(jnp.int32),
        "ray_count": place_ends(jax.random.randint(seeds[5], (RAYS,), NZ // 4, NZ // 2 + CZ + 1), jax.random.fold_in(seeds[5], 1), NZ // 4, (NZ // 2 + CZ + 1) - 1).astype(jnp.int32),
        "target": jnp.clip(1.0 * jax.random.uniform(seeds[6], (3, RAYS), jnp.float32) ** block_levels(seeds[6], (3, RAYS), ((1, 8),), -0.2, 0.2), 0.0, 1.0),
    }


RENDER_WEIGHT = 1000.0
TV_WEIGHT = 0.05
BACKGROUND = 1.0
STEP_SPAN = 4.0
CLIP_RMS = 0.25
LEARN_RATE = 0.02
BETA_ONE = 0.9
BETA_TWO = 0.99
EPSILON = 1e-08

def tile_loss(tile_grid, pixel_index, start_slab, ray_count, target):
    flat = tile_grid.reshape(4, NZ, CX * NY)
    samples = jnp.take(flat, pixel_index, axis=2)
    depth_pos = jnp.arange(NZ, dtype=jnp.int32)[:, None]
    first_cell = start_slab[None, :] * CZ
    inside = (depth_pos >= first_cell) & (depth_pos < first_cell + ray_count[None, :])
    optical = jnp.where(inside, jax.nn.softplus(samples[0]) * (STEP_SPAN / NZ), 0.0)
    running = jnp.cumsum(optical, axis=0)
    weights = jnp.exp(-(running - optical)) * (1.0 - jnp.exp(-optical))
    colors = jax.nn.sigmoid(samples[1:4])
    rendered = lax.optimization_barrier(jnp.sum(weights[None] * colors, axis=1)) + jnp.exp(-running[-1])[None] * BACKGROUND
    return 0.5 * RENDER_WEIGHT * jnp.sum((rendered - target) ** 2)

def reference(voxel_grid, first_moment, second_moment, pixel_index, start_slab, ray_count, target):
    tiles = voxel_grid.reshape(4, NZ, N_TILE, CX, NY).transpose(2, 0, 1, 3, 4)
    pixels = pixel_index.reshape(N_TILE, RAYS_DEV)
    starts = start_slab.reshape(N_TILE, RAYS_DEV)
    counts = ray_count.reshape(N_TILE, RAYS_DEV)
    targets = target.reshape(3, N_TILE, RAYS_DEV).transpose(1, 0, 2)

    def one_tile(inputs):
        return jax.grad(tile_loss)(*inputs)
    tile_grads = lax.map(one_tile, (tiles, pixels, starts, counts, targets))
    render_grad = tile_grads.transpose(1, 2, 0, 3, 4).reshape(4, NZ, NX, NY)
    smooth = jnp.zeros_like(voxel_grid)
    for axis_num in (1, 2, 3):
        step_diff = jnp.diff(voxel_grid, axis=axis_num)
        low_pad = [(0, 0)] * 4
        high_pad = [(0, 0)] * 4
        low_pad[axis_num] = (0, 1)
        high_pad[axis_num] = (1, 0)
        smooth = smooth + jnp.pad(-step_diff, low_pad) + jnp.pad(step_diff, high_pad)
    gradient = render_grad + 2.0 * TV_WEIGHT * smooth
    norm_value = jnp.sqrt(jnp.sum(gradient * gradient))
    limit = CLIP_RMS * math.sqrt(4.0 * NZ * NX * NY)
    clipped = gradient * (limit / jnp.maximum(norm_value, limit))
    new_first = BETA_ONE * first_moment + (1.0 - BETA_ONE) * clipped
    new_second = BETA_TWO * second_moment + (1.0 - BETA_TWO) * clipped * clipped
    first_hat = new_first / (1.0 - BETA_ONE ** STEP)
    second_hat = new_second / (1.0 - BETA_TWO ** STEP)
    new_grid = voxel_grid - LEARN_RATE * first_hat / (jnp.sqrt(second_hat) + EPSILON)
    return (new_grid, new_first, new_second)
```

```python
import functools
import math

import jax
import jax.numpy as jnp
from jax import lax
from jax.experimental import pallas as pl
from jax.experimental.pallas import tpu as pltpu
from jax.sharding import PartitionSpec as P

STEP = 20
RENDER_WEIGHT = 1000.0
TV_WEIGHT = 0.05
BACKGROUND = 1.0
STEP_SPAN = 4.0
CLIP_RMS = 0.25
LEARN_RATE = 0.02
BETA_ONE = 0.9
BETA_TWO = 0.99
EPSILON = 1e-08
CHUNK = 1024
MESH = pl.DeviceIdType.MESH


def kernel(
    ns, nt, chunk,
    grid_ref, pix_ref, start_ref, count_ref, target_ref,
    grad_ref, norm_ref,
    hi_ref, lo_ref, trans_ref, weight_ref, sig_ref, onehot_ref, row_ref, parts_ref, table_ref,
    edge_ref, xhalo_ref, zhalo_ref, nsend_ref, nrecv_ref,
    part_send, part_recv, halo_send, halo_recv, norm_send, norm_recv,
):
    channels, depth, rx, ry = grid_ref.shape
    rays = pix_ref.shape[1]
    chunks = rays // chunk
    total_depth = depth * ns
    span = STEP_SPAN / total_depth
    rows = depth * rx
    slab = lax.axis_index("slab")
    tile = lax.axis_index("tile")

    def slab_peer(d):
        return {"slab": lax.rem(slab + d, ns)}

    def tile_peer(d):
        return {"tile": lax.rem(tile + d, nt)}

    barrier = pltpu.get_barrier_semaphore()
    for d in range(1, ns):
        pl.semaphore_signal(barrier, inc=1, device_id=slab_peer(d), device_id_type=MESH)
    for d in range(1, nt):
        pl.semaphore_signal(barrier, inc=1, device_id=tile_peer(d), device_id_type=MESH)

    edge_ref[0] = grid_ref[:, :, rx - 1, :]
    edge_ref[1] = grid_ref[:, :, 0, :]

    total = jnp.zeros((rx, ry), jnp.float32)
    before = jnp.ones((rx, ry), jnp.float32)
    sums = [jnp.zeros((rx, ry), jnp.float32) for _ in range(3)]
    for z in range(depth):
        s = grid_ref[0, z]
        e = jnp.exp(-jnp.abs(s))
        tau = (jnp.maximum(s, 0.0) + jnp.log1p(e)) * span
        sig_ref[0, z] = jnp.where(s >= 0, 1.0, e) / (1.0 + e)
        total = total + tau
        after = jnp.exp(-total)
        w = before * (1.0 - jnp.exp(-tau))
        before = after
        trans_ref[z] = after
        weight_ref[z] = w
        for c in range(3):
            col = 1.0 / (1.0 + jnp.exp(-grid_ref[c + 1, z]))
            sig_ref[c + 1, z] = col
            sums[c] = sums[c] + w * col
            table_ref[pl.ds(c * rows + z * rx, rx), :] = sums[c]
        table_ref[pl.ds(3 * rows + z * rx, rx), :] = after
    full = table_ref[...]
    high = full.astype(jnp.bfloat16)
    hi_ref[...] = high
    lo_ref[...] = (full - high.astype(jnp.float32)).astype(jnp.bfloat16)

    pl.semaphore_wait(barrier, ns - 1 + nt - 1)

    halos = [
        pltpu.make_async_remote_copy(
            src_ref=grid_ref.at[:, depth - 1], dst_ref=zhalo_ref.at[0],
            send_sem=halo_send.at[0], recv_sem=halo_recv.at[0],
            device_id=slab_peer(1), device_id_type=MESH),
        pltpu.make_async_remote_copy(
            src_ref=grid_ref.at[:, 0], dst_ref=zhalo_ref.at[1],
            send_sem=halo_send.at[1], recv_sem=halo_recv.at[1],
            device_id=slab_peer(ns - 1), device_id_type=MESH),
        pltpu.make_async_remote_copy(
            src_ref=edge_ref.at[0], dst_ref=xhalo_ref.at[0],
            send_sem=halo_send.at[2], recv_sem=halo_recv.at[2],
            device_id=tile_peer(1), device_id_type=MESH),
        pltpu.make_async_remote_copy(
            src_ref=edge_ref.at[1], dst_ref=xhalo_ref.at[1],
            send_sem=halo_send.at[3], recv_sem=halo_recv.at[3],
            device_id=tile_peer(nt - 1), device_id_type=MESH),
    ]

    def part_copy(d, j):
        return pltpu.make_async_remote_copy(
            src_ref=parts_ref.at[slab, j], dst_ref=parts_ref.at[slab, j],
            send_sem=part_send.at[d - 1, j], recv_sem=part_recv.at[d - 1, j],
            device_id=slab_peer(d), device_id_type=MESH)

    def part_wait(d, j):
        source = lax.rem(slab + ns - d, ns)
        pltpu.make_async_remote_copy(
            src_ref=parts_ref.at[source, j], dst_ref=parts_ref.at[source, j],
            send_sem=part_send.at[d - 1, j], recv_sem=part_recv.at[d - 1, j],
            device_id=slab_peer(d), device_id_type=MESH).wait_recv()

    y_ids = lax.broadcasted_iota(jnp.int32, (ry, chunk), 0).astype(jnp.float32).astype(jnp.bfloat16)
    row_ids = lax.broadcasted_iota(jnp.int32, (rows, chunk), 0)

    for j in range(chunks):
        at = pl.ds(j * chunk, chunk)
        pix = pix_ref[:, at]
        start = start_ref[:, at]
        px = pix // ry
        py = (pix - px * ry).astype(jnp.float32).astype(jnp.bfloat16)
        length = jnp.clip((start - slab) * depth + count_ref[:, at], 0, depth)
        length = jnp.where(slab >= start, length, 0)
        row = jnp.where(length > 0, (length - 1) * rx + px, -1)
        row_ref[:, at] = row
        hot = jnp.where(y_ids == py, jnp.ones((), jnp.bfloat16), jnp.zeros((), jnp.bfloat16))
        onehot_ref[:, at] = hot
        mask = row_ids == row
        for c in range(4):
            block = pl.ds(c * rows, rows)
            u = jnp.dot(hi_ref[block, :], hot, preferred_element_type=jnp.float32)
            u = u + jnp.dot(lo_ref[block, :], hot, preferred_element_type=jnp.float32)
            part = jnp.sum(jnp.where(mask, u, 0.0), axis=0, keepdims=True)
            if c == 3:
                part = jnp.where(row < 0, 1.0, part)
            parts_ref[slab, j, pl.ds(c, 1), :] = part
        for d in range(1, ns):
            part_copy(d, j).start()
        if j == 0:
            for h in halos:
                h.start()

    for h in halos:
        h.wait_recv()
    x_ids = lax.broadcasted_iota(jnp.int32, (rx, ry), 0)
    lane_ids = lax.broadcasted_iota(jnp.int32, (rx, ry), 1)
    first_x = tile == 0
    last_x = tile == nt - 1
    for c in range(channels):
        for z in range(depth):
            g = grid_ref[c, z]
            if z > 0:
                below = grid_ref[c, z - 1]
            else:
                below = jnp.where(slab > 0, zhalo_ref[0, c], g)
            if z < depth - 1:
                above = grid_ref[c, z + 1]
            else:
                above = jnp.where(slab < ns - 1, zhalo_ref[1, c], g)
            xl = jnp.broadcast_to(xhalo_ref[0, c, pl.ds(z, 1), :], (rx, ry))
            xh = jnp.broadcast_to(xhalo_ref[1, c, pl.ds(z, 1), :], (rx, ry))
            xl = jnp.where(first_x, g, xl)
            xh = jnp.where(last_x, g, xh)
            left = jnp.where(x_ids == 0, xl, pltpu.roll(g, 1, 0))
            right = jnp.where(x_ids == rx - 1, xh, pltpu.roll(g, rx - 1, 0))
            down = jnp.where(lane_ids == 0, g, pltpu.roll(g, 1, 1))
            up = jnp.where(lane_ids == ry - 1, g, pltpu.roll(g, ry - 1, 1))
            smooth = (g - below) + (g - above) + (g - left) + (g - right) + (g - down) + (g - up)
            grad_ref[c, z] = (2.0 * TV_WEIGHT) * smooth

    row_ids16 = row_ids
    for j in range(chunks):
        for d in range(1, ns):
            part_wait(d, j)
        at = pl.ds(j * chunk, chunk)
        front_c = jnp.zeros((3, chunk), jnp.float32)
        front_t = jnp.ones((1, chunk), jnp.float32)
        beyond = jnp.full((3, chunk), BACKGROUND, jnp.float32)
        for s in range(ns - 1):
            here = slab > s
            pc = parts_ref[s, j, pl.ds(0, 3), :]
            pt = parts_ref[s, j, pl.ds(3, 1), :]
            front_c = jnp.where(here, front_c + front_t * pc, front_c)
            front_t = jnp.where(here, front_t * pt, front_t)
        for s in range(ns - 1, 0, -1):
            here = slab < s
            pc = parts_ref[s, j, pl.ds(0, 3), :]
            pt = parts_ref[s, j, pl.ds(3, 1), :]
            beyond = jnp.where(here, pc + pt * beyond, beyond)
        pc = parts_ref[slab, j, pl.ds(0, 3), :]
        pt = parts_ref[slab, j, pl.ds(3, 1), :]
        rendered = front_c + front_t * (pc + pt * beyond)
        residual = RENDER_WEIGHT * (rendered - target_ref[:, at])
        color_cot = front_t * residual
        trans_cot = front_t * jnp.sum(residual * beyond, axis=0, keepdims=True)
        hot = onehot_ref[:, at]
        mask = row_ids16 == row_ref[:, at]
        for c in range(4):
            cot = color_cot[c:c + 1] if c < 3 else trans_cot
            spread = jnp.where(mask, cot, 0.0)
            top = spread.astype(jnp.bfloat16)
            rest = (spread - top.astype(jnp.float32)).astype(jnp.bfloat16)
            dims = (((1,), (1,)), ((), ()))
            u = lax.dot_general(top, hot, dims, preferred_element_type=jnp.float32)
            u = u + lax.dot_general(rest, hot, dims, preferred_element_type=jnp.float32)
            block = pl.ds(c * rows, rows)
            if j == 0:
                table_ref[block, :] = u
            else:
                table_ref[block, :] += u

    zero = jnp.zeros((rx, ry), jnp.float32)
    suffix = [zero, zero, zero]
    later = zero
    squares = zero
    for z in range(depth - 1, -1, -1):
        w = weight_ref[z]
        after = trans_ref[z]
        later = later + after * table_ref[pl.ds(3 * rows + z * rx, rx), :]
        dw = zero
        for c in range(3):
            suffix[c] = suffix[c] + table_ref[pl.ds(c * rows + z * rx, rx), :]
            col = sig_ref[c + 1, z]
            dw = dw + col * suffix[c]
            out = grad_ref[c + 1, z] + w * suffix[c] * (col * (1.0 - col))
            grad_ref[c + 1, z] = out
            squares = squares + out * out
        dtau = after * dw - later
        later = later + w * dw
        out = grad_ref[0, z] + dtau * (sig_ref[0, z] * span)
        grad_ref[0, z] = out
        squares = squares + out * out

    local = jnp.sum(squares)

    def norm_copy(phase, d, slot, peer):
        return pltpu.make_async_remote_copy(
            src_ref=nsend_ref.at[phase], dst_ref=nrecv_ref.at[slot],
            send_sem=norm_send.at[slot], recv_sem=norm_recv.at[slot],
            device_id=peer, device_id_type=MESH)

    value = jnp.full((8, 128), local, jnp.float32)
    copies = []
    for phase, count, peer in ((0, nt, tile_peer), (1, ns, slab_peer)):
        nsend_ref[phase] = value
        base = 0 if phase == 0 else nt - 1
        group = [norm_copy(phase, d, base + d - 1, peer(d)) for d in range(1, count)]
        for copy in group:
            copy.start()
        for i, copy in enumerate(group):
            copy.wait_recv()
            value = value + nrecv_ref[base + i]
        copies += group
    norm_ref[...] = value
    for copy in copies:
        copy.wait_send()
    for h in halos:
        h.wait_send()
    for j in range(chunks):
        for d in range(1, ns):
            part_copy(d, j).wait_send()


def per_device(voxel_grid, first_moment, second_moment, pixel_index, start_slab, ray_count, target):
    ns = lax.axis_size("slab")
    nt = lax.axis_size("tile")
    channels, depth, rx, ry = voxel_grid.shape
    rays = pixel_index.shape[0]
    chunk = math.gcd(rays, CHUNK)
    chunks = rays // chunk
    rows = depth * rx
    f32 = jnp.float32
    vmem = pl.BlockSpec(memory_space=pltpu.VMEM)
    gradient, square_sum = pl.pallas_call(
        functools.partial(kernel, ns, nt, chunk),
        out_shape=(
            jax.ShapeDtypeStruct(voxel_grid.shape, f32),
            jax.ShapeDtypeStruct((8, 128), f32),
        ),
        in_specs=[vmem] * 5,
        out_specs=(vmem, vmem),
        scratch_shapes=[
            pltpu.VMEM((channels * rows, ry), jnp.bfloat16),
            pltpu.VMEM((channels * rows, ry), jnp.bfloat16),
            pltpu.VMEM((depth, rx, ry), f32),
            pltpu.VMEM((depth, rx, ry), f32),
            pltpu.VMEM((channels, depth, rx, ry), f32),
            pltpu.VMEM((ry, rays), jnp.bfloat16),
            pltpu.VMEM((1, rays), jnp.int32),
            pltpu.VMEM((ns, chunks, 4, chunk), f32),
            pltpu.VMEM((channels * rows, ry), f32),
            pltpu.VMEM((2, channels, depth, ry), f32),
            pltpu.VMEM((2, channels, depth, ry), f32),
            pltpu.VMEM((2, channels, rx, ry), f32),
            pltpu.VMEM((2, 8, 128), f32),
            pltpu.VMEM((nt + ns - 2, 8, 128), f32),
            pltpu.SemaphoreType.DMA((ns - 1, chunks)),
            pltpu.SemaphoreType.DMA((ns - 1, chunks)),
            pltpu.SemaphoreType.DMA((4,)),
            pltpu.SemaphoreType.DMA((4,)),
            pltpu.SemaphoreType.DMA((nt + ns - 2,)),
            pltpu.SemaphoreType.DMA((nt + ns - 2,)),
        ],
        compiler_params=pltpu.CompilerParams(
            collective_id=0, has_side_effects=True, vmem_limit_bytes=32 * 1024 * 1024
        ),
        name="render_step",
    )(
        voxel_grid,
        pixel_index.reshape(1, rays),
        start_slab.reshape(1, rays),
        ray_count.reshape(1, rays),
        target,
    )
    norm_value = jnp.sqrt(square_sum[0, 0])
    limit = CLIP_RMS * math.sqrt(4.0 * (depth * ns) * (rx * nt) * ry)
    clipped = gradient * (limit / jnp.maximum(norm_value, limit))
    new_first = BETA_ONE * first_moment + (1.0 - BETA_ONE) * clipped
    new_second = BETA_TWO * second_moment + (1.0 - BETA_TWO) * clipped * clipped
    first_hat = new_first / (1.0 - BETA_ONE**STEP)
    second_hat = new_second / (1.0 - BETA_TWO**STEP)
    new_grid = voxel_grid - LEARN_RATE * first_hat / (jnp.sqrt(second_hat) + EPSILON)
    return (new_grid, new_first, new_second)


def solution(mesh):
    cells = P(None, "slab", "tile", None)
    return jax.shard_map(
        per_device,
        mesh=mesh,
        in_specs=(cells, cells, cells, P("tile"), P("tile"), P("tile"), P(None, "tile")),
        out_specs=(cells, cells, cells),
        check_vma=False,
    )
```

```python
import functools
import math

import jax
import jax.numpy as jnp
from jax import lax
from jax.experimental import pallas as pl
from jax.experimental.pallas import tpu as pltpu
from jax.sharding import PartitionSpec as P

STEP = 20
RENDER_WEIGHT = 1000.0
TV_WEIGHT = 0.05
BACKGROUND = 1.0
STEP_SPAN = 4.0
CLIP_RMS = 0.25
LEARN_RATE = 0.02
BETA_ONE = 0.9
BETA_TWO = 0.99
EPSILON = 1e-08
CHUNK = 1024
MESH = pl.DeviceIdType.MESH


def kernel(
    ns, nt, chunk,
    grid_hbm, first_hbm, second_hbm, pix_hbm, start_hbm, count_hbm, target_hbm,
    grid_ref, first_ref, second_ref, grad_ref, scale_ref,
    pix_ref, start_ref, count_ref, target_ref,
    pair_ref, trans_ref, weight_ref, sig_ref, onehot_ref, row_ref, parts_ref, table_ref,
    edge_ref, xhalo_ref, zhalo_ref, nsend_ref, nrecv_ref,
    part_send, part_recv, halo_send, halo_recv, norm_send, norm_recv, load_sem,
):
    channels, depth, rx, ry = grid_ref.shape
    rays = pix_ref.shape[1]
    chunks = rays // chunk
    total_depth = depth * ns
    span = STEP_SPAN / total_depth
    rows = depth * rx
    slab = lax.axis_index("slab")
    tile = lax.axis_index("tile")

    def slab_peer(d):
        return {"slab": lax.rem(slab + d, ns)}

    def tile_peer(d):
        return {"tile": lax.rem(tile + d, nt)}

    loads = [
        pltpu.make_async_copy(grid_hbm.at[c], grid_ref.at[c], load_sem.at[c])
        for c in range(channels)
    ]
    rest = (
        (pix_hbm, pix_ref), (start_hbm, start_ref), (count_hbm, count_ref),
        (target_hbm, target_ref), (first_hbm, first_ref), (second_hbm, second_ref),
    )
    loads += [
        pltpu.make_async_copy(a, b, load_sem.at[channels + i]) for i, (a, b) in enumerate(rest)
    ]
    for copy in loads:
        copy.start()

    barrier = pltpu.get_barrier_semaphore()
    for d in range(1, ns):
        pl.semaphore_signal(barrier, inc=1, device_id=slab_peer(d), device_id_type=MESH)
    for d in range(1, nt):
        pl.semaphore_signal(barrier, inc=1, device_id=tile_peer(d), device_id_type=MESH)

    for c in range(channels):
        loads[c].wait()
    edge_ref[0] = grid_ref[:, :, rx - 1, :]
    edge_ref[1] = grid_ref[:, :, 0, :]

    total = jnp.zeros((rx, ry), jnp.float32)
    before = jnp.ones((rx, ry), jnp.float32)
    sums = [jnp.zeros((rx, ry), jnp.float32) for _ in range(3)]
    for z in range(depth):
        s = grid_ref[0, z]
        e = jnp.exp(-jnp.abs(s))
        tau = (jnp.maximum(s, 0.0) + jnp.log1p(e)) * span
        sig_ref[0, z] = jnp.where(s >= 0, 1.0, e) / (1.0 + e)
        total = total + tau
        after = jnp.exp(-total)
        w = before * (1.0 - jnp.exp(-tau))
        before = after
        trans_ref[z] = after
        weight_ref[z] = w
        for c in range(3):
            col = 1.0 / (1.0 + jnp.exp(-grid_ref[c + 1, z]))
            sig_ref[c + 1, z] = col
            sums[c] = sums[c] + w * col
            table_ref[pl.ds(c * rows + z * rx, rx), :] = sums[c]
        table_ref[pl.ds(3 * rows + z * rx, rx), :] = after
    full = table_ref[...]
    high = full.astype(jnp.bfloat16)
    pair_ref[:, :ry] = high
    pair_ref[:, ry:] = (full - high.astype(jnp.float32)).astype(jnp.bfloat16)

    pl.semaphore_wait(barrier, ns - 1 + nt - 1)

    def halo_copy(src, dst, i, peer):
        return pltpu.make_async_remote_copy(
            src_ref=src, dst_ref=dst, send_sem=halo_send.at[i], recv_sem=halo_recv.at[i],
            device_id=peer, device_id_type=MESH)

    halos = [
        (halo_copy(grid_ref.at[:, depth - 1], zhalo_ref.at[0], 0, slab_peer(1)), slab < ns - 1, slab > 0),
        (halo_copy(grid_ref.at[:, 0], zhalo_ref.at[1], 1, slab_peer(ns - 1)), slab > 0, slab < ns - 1),
        (halo_copy(edge_ref.at[0], xhalo_ref.at[0], 2, tile_peer(1)), tile < nt - 1, tile > 0),
        (halo_copy(edge_ref.at[1], xhalo_ref.at[1], 3, tile_peer(nt - 1)), tile > 0, tile < nt - 1),
    ]
    for copy, sends, _ in halos:
        pl.when(sends)(copy.start)

    def part_copy(d, j):
        return pltpu.make_async_remote_copy(
            src_ref=parts_ref.at[slab, j], dst_ref=parts_ref.at[slab, j],
            send_sem=part_send.at[d - 1, j], recv_sem=part_recv.at[d - 1, j],
            device_id=slab_peer(d), device_id_type=MESH)

    def part_wait(d, j):
        source = lax.rem(slab + ns - d, ns)
        pltpu.make_async_remote_copy(
            src_ref=parts_ref.at[source, j], dst_ref=parts_ref.at[source, j],
            send_sem=part_send.at[d - 1, j], recv_sem=part_recv.at[d - 1, j],
            device_id=slab_peer(d), device_id_type=MESH).wait_recv()

    y_ids = lax.broadcasted_iota(jnp.int32, (ry, chunk), 0).astype(jnp.float32).astype(jnp.bfloat16)
    row_ids = lax.broadcasted_iota(jnp.int32, (rows, chunk), 0)

    for copy in loads[channels:channels + 3]:
        copy.wait()
    for j in range(chunks):
        at = pl.ds(j * chunk, chunk)
        pix = pix_ref[:, at]
        start = start_ref[:, at]
        px = pix // ry
        py = (pix - px * ry).astype(jnp.float32).astype(jnp.bfloat16)
        length = jnp.clip((start - slab) * depth + count_ref[:, at], 0, depth)
        length = jnp.where(slab >= start, length, 0)
        row = jnp.where(length > 0, (length - 1) * rx + px, -1)
        row_ref[:, at] = row
        hot = jnp.where(y_ids == py, jnp.ones((), jnp.bfloat16), jnp.zeros((), jnp.bfloat16))
        onehot_ref[:, at] = hot
        twice = jnp.concatenate([hot, hot], axis=0)
        mask = row_ids == row
        for c in range(4):
            block = pl.ds(c * rows, rows)
            u = jnp.dot(pair_ref[block, :], twice, preferred_element_type=jnp.float32)
            part = jnp.sum(jnp.where(mask, u, 0.0), axis=0, keepdims=True)
            if c == 3:
                part = jnp.where(row < 0, 1.0, part)
            parts_ref[slab, j, pl.ds(c, 1), :] = part
        for d in range(1, ns):
            part_copy(d, j).start()

    for copy, _, receives in halos:
        pl.when(receives)(copy.wait_recv)
    x_ids = lax.broadcasted_iota(jnp.int32, (rx, ry), 0)
    lane_ids = lax.broadcasted_iota(jnp.int32, (rx, ry), 1)
    first_x = tile == 0
    last_x = tile == nt - 1
    for c in range(channels):
        for z in range(depth):
            g = grid_ref[c, z]
            if z > 0:
                below = grid_ref[c, z - 1]
            else:
                below = jnp.where(slab > 0, zhalo_ref[0, c], g)
            if z < depth - 1:
                above = grid_ref[c, z + 1]
            else:
                above = jnp.where(slab < ns - 1, zhalo_ref[1, c], g)
            xl = jnp.broadcast_to(xhalo_ref[0, c, pl.ds(z, 1), :], (rx, ry))
            xh = jnp.broadcast_to(xhalo_ref[1, c, pl.ds(z, 1), :], (rx, ry))
            xl = jnp.where(first_x, g, xl)
            xh = jnp.where(last_x, g, xh)
            left = jnp.where(x_ids == 0, xl, pltpu.roll(g, 1, 0))
            right = jnp.where(x_ids == rx - 1, xh, pltpu.roll(g, rx - 1, 0))
            down = jnp.where(lane_ids == 0, g, pltpu.roll(g, 1, 1))
            up = jnp.where(lane_ids == ry - 1, g, pltpu.roll(g, ry - 1, 1))
            smooth = (g - below) + (g - above) + (g - left) + (g - right) + (g - down) + (g - up)
            grad_ref[c, z] = (2.0 * TV_WEIGHT) * smooth

    loads[channels + 3].wait()
    row_ids16 = row_ids.astype(jnp.float32).astype(jnp.bfloat16)
    for j in range(chunks):
        for d in range(1, ns):
            part_wait(d, j)
        at = pl.ds(j * chunk, chunk)
        front_c = jnp.zeros((3, chunk), jnp.float32)
        front_t = jnp.ones((1, chunk), jnp.float32)
        beyond = jnp.full((3, chunk), BACKGROUND, jnp.float32)
        for s in range(ns - 1):
            here = slab > s
            pc = parts_ref[s, j, pl.ds(0, 3), :]
            pt = parts_ref[s, j, pl.ds(3, 1), :]
            front_c = jnp.where(here, front_c + front_t * pc, front_c)
            front_t = jnp.where(here, front_t * pt, front_t)
        for s in range(ns - 1, 0, -1):
            here = slab < s
            pc = parts_ref[s, j, pl.ds(0, 3), :]
            pt = parts_ref[s, j, pl.ds(3, 1), :]
            beyond = jnp.where(here, pc + pt * beyond, beyond)
        pc = parts_ref[slab, j, pl.ds(0, 3), :]
        pt = parts_ref[slab, j, pl.ds(3, 1), :]
        rendered = front_c + front_t * (pc + pt * beyond)
        residual = RENDER_WEIGHT * (rendered - target_ref[:, at])
        color_cot = front_t * residual
        trans_cot = front_t * jnp.sum(residual * beyond, axis=0, keepdims=True)
        hot = onehot_ref[:, at]
        twice = jnp.concatenate([hot, hot], axis=1)
        mask = row_ids16 == row_ref[:, at].astype(jnp.float32).astype(jnp.bfloat16)
        none = jnp.zeros((), jnp.bfloat16)
        for c in range(4):
            cot = color_cot[c:c + 1] if c < 3 else trans_cot
            top = cot.astype(jnp.bfloat16)
            low = (cot - top.astype(jnp.float32)).astype(jnp.bfloat16)
            spread = jnp.concatenate(
                [jnp.where(mask, top, none), jnp.where(mask, low, none)], axis=1)
            u = lax.dot_general(
                spread, twice, (((1,), (1,)), ((), ())), preferred_element_type=jnp.float32)
            block = pl.ds(c * rows, rows)
            if j == 0:
                table_ref[block, :] = u
            else:
                table_ref[block, :] += u

    zero = jnp.zeros((rx, ry), jnp.float32)
    suffix = [zero, zero, zero]
    later = zero
    squares = zero
    for z in range(depth - 1, -1, -1):
        w = weight_ref[z]
        after = trans_ref[z]
        later = later + after * table_ref[pl.ds(3 * rows + z * rx, rx), :]
        dw = zero
        for c in range(3):
            suffix[c] = suffix[c] + table_ref[pl.ds(c * rows + z * rx, rx), :]
            col = sig_ref[c + 1, z]
            dw = dw + col * suffix[c]
            out = grad_ref[c + 1, z] + w * suffix[c] * (col * (1.0 - col))
            grad_ref[c + 1, z] = out
            squares = squares + out * out
        dtau = after * dw - later
        later = later + w * dw
        out = grad_ref[0, z] + dtau * (sig_ref[0, z] * span)
        grad_ref[0, z] = out
        squares = squares + out * out

    local = jnp.sum(squares)

    def norm_copy(phase, d, slot, peer):
        return pltpu.make_async_remote_copy(
            src_ref=nsend_ref.at[phase], dst_ref=nrecv_ref.at[slot],
            send_sem=norm_send.at[slot], recv_sem=norm_recv.at[slot],
            device_id=peer, device_id_type=MESH)

    value = jnp.full((8, 128), local, jnp.float32)
    copies = []
    for phase, count, peer in ((0, nt, tile_peer), (1, ns, slab_peer)):
        nsend_ref[phase] = value
        base = 0 if phase == 0 else nt - 1
        group = [norm_copy(phase, d, base + d - 1, peer(d)) for d in range(1, count)]
        for copy in group:
            copy.start()
        for i, copy in enumerate(group):
            copy.wait_recv()
            value = value + nrecv_ref[base + i]
        copies += group
    limit = CLIP_RMS * math.sqrt(4.0 * total_depth * (rx * nt) * ry)
    scale_ref[...] = limit / jnp.maximum(jnp.sqrt(value), limit)
    for copy in loads[channels + 4:]:
        copy.wait()
    for copy in copies:
        copy.wait_send()
    for copy, sends, _ in halos:
        pl.when(sends)(copy.wait_send)
    for j in range(chunks):
        for d in range(1, ns):
            part_copy(d, j).wait_send()


def adam_kernel(
    grid_ref, first_ref, second_ref, grad_ref, scale_ref,
    grid_hbm, first_hbm, second_hbm, grid_out, first_out, second_out, sem,
):
    channels, depth, rx, ry = grid_ref.shape
    scale = jnp.broadcast_to(scale_ref[0:1, 0:1], (rx, ry))
    copies = []
    for c in range(channels):
        for z in range(depth):
            clipped = grad_ref[c, z] * scale
            first = BETA_ONE * first_ref[c, z] + (1.0 - BETA_ONE) * clipped
            second = BETA_TWO * second_ref[c, z] + (1.0 - BETA_TWO) * clipped * clipped
            first_out[c, z] = first
            second_out[c, z] = second
            first_hat = first * (1.0 / (1.0 - BETA_ONE**STEP))
            second_hat = second * (1.0 / (1.0 - BETA_TWO**STEP))
            grid_out[c, z] = grid_ref[c, z] - LEARN_RATE * first_hat / (
                jnp.sqrt(second_hat) + EPSILON)
        pairs = ((first_out, first_hbm), (second_out, second_hbm), (grid_out, grid_hbm))
        for i, (a, b) in enumerate(pairs):
            copy = pltpu.make_async_copy(a.at[c], b.at[c], sem.at[i, c])
            copy.start()
            copies.append(copy)
    for copy in copies:
        copy.wait()


def per_device(voxel_grid, first_moment, second_moment, pixel_index, start_slab, ray_count, target):
    ns = lax.axis_size("slab")
    nt = lax.axis_size("tile")
    channels, depth, rx, ry = voxel_grid.shape
    rays = pixel_index.shape[0]
    chunk = math.gcd(rays, CHUNK)
    chunks = rays // chunk
    rows = depth * rx
    f32 = jnp.float32
    vmem = pl.BlockSpec(memory_space=pltpu.VMEM)
    hbm = pl.BlockSpec(memory_space=pltpu.HBM)
    cells = jax.ShapeDtypeStruct(voxel_grid.shape, f32)
    staged = pl.pallas_call(
        functools.partial(kernel, ns, nt, chunk),
        out_shape=(cells, cells, cells, cells, jax.ShapeDtypeStruct((8, 128), f32)),
        in_specs=[hbm] * 7,
        out_specs=(vmem,) * 5,
        scratch_shapes=[
            pltpu.VMEM((1, rays), jnp.int32),
            pltpu.VMEM((1, rays), jnp.int32),
            pltpu.VMEM((1, rays), jnp.int32),
            pltpu.VMEM(target.shape, f32),
            pltpu.VMEM((channels * rows, 2 * ry), jnp.bfloat16),
            pltpu.VMEM((depth, rx, ry), f32),
            pltpu.VMEM((depth, rx, ry), f32),
            pltpu.VMEM((channels, depth, rx, ry), f32),
            pltpu.VMEM((ry, rays), jnp.bfloat16),
            pltpu.VMEM((1, rays), jnp.int32),
            pltpu.VMEM((ns, chunks, 4, chunk), f32),
            pltpu.VMEM((channels * rows, ry), f32),
            pltpu.VMEM((2, channels, depth, ry), f32),
            pltpu.VMEM((2, channels, depth, ry), f32),
            pltpu.VMEM((2, channels, rx, ry), f32),
            pltpu.VMEM((2, 8, 128), f32),
            pltpu.VMEM((nt + ns - 2, 8, 128), f32),
            pltpu.SemaphoreType.DMA((ns - 1, chunks)),
            pltpu.SemaphoreType.DMA((ns - 1, chunks)),
            pltpu.SemaphoreType.DMA((4,)),
            pltpu.SemaphoreType.DMA((4,)),
            pltpu.SemaphoreType.DMA((nt + ns - 2,)),
            pltpu.SemaphoreType.DMA((nt + ns - 2,)),
            pltpu.SemaphoreType.DMA((channels + 6,)),
        ],
        compiler_params=pltpu.CompilerParams(
            collective_id=0, has_side_effects=True, vmem_limit_bytes=32 * 1024 * 1024
        ),
        name="render_step",
    )(*(pltpu.with_memory_space_constraint(a, pltpu.HBM) for a in (
        voxel_grid,
        first_moment,
        second_moment,
        pixel_index.reshape(1, rays),
        start_slab.reshape(1, rays),
        ray_count.reshape(1, rays),
        target,
    )))
    return pl.pallas_call(
        adam_kernel,
        out_shape=(cells, cells, cells),
        in_specs=[vmem] * 5,
        out_specs=(hbm, hbm, hbm),
        scratch_shapes=[
            pltpu.VMEM(voxel_grid.shape, f32),
            pltpu.VMEM(voxel_grid.shape, f32),
            pltpu.VMEM(voxel_grid.shape, f32),
            pltpu.SemaphoreType.DMA((3, channels)),
        ],
        compiler_params=pltpu.CompilerParams(vmem_limit_bytes=32 * 1024 * 1024),
        name="adam",
    )(*staged)


def solution(mesh):
    cells = P(None, "slab", "tile", None)
    return jax.shard_map(
        per_device,
        mesh=mesh,
        in_specs=(cells, cells, cells, P("tile"), P("tile"), P("tile"), P(None, "tile")),
        out_specs=(cells, cells, cells),
        check_vma=False,
    )
```

```python
import functools
import math

import jax
import jax.numpy as jnp
from jax import lax
from jax.experimental import pallas as pl
from jax.experimental.pallas import tpu as pltpu
from jax.sharding import PartitionSpec as P

STEP = 20
RENDER_WEIGHT = 1000.0
TV_WEIGHT = 0.05
BACKGROUND = 1.0
STEP_SPAN = 4.0
CLIP_RMS = 0.25
LEARN_RATE = 0.02
BETA_ONE = 0.9
BETA_TWO = 0.99
EPSILON = 1e-08
CHUNK = 512
DIRECT_LIMIT = 64
MESH = pl.DeviceIdType.MESH


def kernel(
    ns, nt, chunk,
    grid_hbm, first_hbm, second_hbm, pix_hbm, start_hbm, count_hbm, target_hbm,
    grid_ref, first_ref, second_ref, grad_ref, scale_ref,
    pix_ref, start_ref, count_ref, target_ref,
    pair_ref, trans_ref, weight_ref, sig_ref, onehot_ref, row_ref, parts_ref, table_ref,
    edge_ref, xhalo_ref, zhalo_ref, nsend_ref, nrecv_ref,
    part_send, part_recv, halo_send, halo_recv, norm_send, norm_recv, load_sem,
):
    channels, depth, rx, ry = grid_ref.shape
    rays = pix_ref.shape[1]
    chunks = rays // chunk
    total_depth = depth * ns
    span = STEP_SPAN / total_depth
    rows = depth * rx
    slab = lax.axis_index("slab")
    tile = lax.axis_index("tile")

    def slab_peer(d):
        return {"slab": lax.rem(slab + d, ns)}

    def tile_peer(d):
        return {"tile": lax.rem(tile + d, nt)}

    if direct(ns, nt):
        phases = [[
            {"slab": lax.rem(slab + k // nt, ns), "tile": lax.rem(tile + k % nt, nt)}
            for k in range(1, ns * nt)
        ]]
        greeted = phases[0]
    else:
        phases = [[tile_peer(d) for d in range(1, nt)], [slab_peer(d) for d in range(1, ns)]]
        greeted = phases[0] + phases[1]

    loads = [
        pltpu.make_async_copy(grid_hbm.at[c], grid_ref.at[c], load_sem.at[c])
        for c in range(channels)
    ]
    rest = (
        (pix_hbm, pix_ref), (start_hbm, start_ref), (count_hbm, count_ref),
        (target_hbm, target_ref), (first_hbm, first_ref), (second_hbm, second_ref),
    )
    loads += [
        pltpu.make_async_copy(a, b, load_sem.at[channels + i]) for i, (a, b) in enumerate(rest)
    ]
    for copy in loads:
        copy.start()

    barrier = pltpu.get_barrier_semaphore()
    for peer in greeted:
        pl.semaphore_signal(barrier, inc=1, device_id=peer, device_id_type=MESH)

    for c in range(channels):
        loads[c].wait()
    edge_ref[0] = grid_ref[:, :, rx - 1, :]
    edge_ref[1] = grid_ref[:, :, 0, :]

    total = jnp.zeros((rx, ry), jnp.float32)
    before = jnp.ones((rx, ry), jnp.float32)
    sums = [jnp.zeros((rx, ry), jnp.float32) for _ in range(3)]
    for z in range(depth):
        s = grid_ref[0, z]
        e = jnp.exp(-jnp.abs(s))
        tau = (jnp.maximum(s, 0.0) + jnp.log1p(e)) * span
        sig_ref[0, z] = jnp.where(s >= 0, 1.0, e) / (1.0 + e)
        total = total + tau
        after = jnp.exp(-total)
        w = before * (1.0 - jnp.exp(-tau))
        before = after
        trans_ref[z] = after
        weight_ref[z] = w
        for c in range(3):
            col = 1.0 / (1.0 + jnp.exp(-grid_ref[c + 1, z]))
            sig_ref[c + 1, z] = col
            sums[c] = sums[c] + w * col
            table_ref[pl.ds(c * rows + z * rx, rx), :] = sums[c]
        table_ref[pl.ds(3 * rows + z * rx, rx), :] = after
    full = table_ref[...]
    high = full.astype(jnp.bfloat16)
    pair_ref[:, :ry] = high
    pair_ref[:, ry:] = (full - high.astype(jnp.float32)).astype(jnp.bfloat16)

    pl.semaphore_wait(barrier, len(greeted))

    def halo_copy(src, dst, i, peer):
        return pltpu.make_async_remote_copy(
            src_ref=src, dst_ref=dst, send_sem=halo_send.at[i], recv_sem=halo_recv.at[i],
            device_id=peer, device_id_type=MESH)

    halos = [
        (halo_copy(grid_ref.at[:, depth - 1], zhalo_ref.at[0], 0, slab_peer(1)), slab < ns - 1, slab > 0),
        (halo_copy(grid_ref.at[:, 0], zhalo_ref.at[1], 1, slab_peer(ns - 1)), slab > 0, slab < ns - 1),
        (halo_copy(edge_ref.at[0], xhalo_ref.at[0], 2, tile_peer(1)), tile < nt - 1, tile > 0),
        (halo_copy(edge_ref.at[1], xhalo_ref.at[1], 3, tile_peer(nt - 1)), tile > 0, tile < nt - 1),
    ]
    for copy, sends, _ in halos:
        pl.when(sends)(copy.start)

    def part_copy(d, j):
        return pltpu.make_async_remote_copy(
            src_ref=parts_ref.at[slab, j], dst_ref=parts_ref.at[slab, j],
            send_sem=part_send.at[d - 1, j], recv_sem=part_recv.at[d - 1, j],
            device_id=slab_peer(d), device_id_type=MESH)

    def part_wait(d, j):
        source = lax.rem(slab + ns - d, ns)
        pltpu.make_async_remote_copy(
            src_ref=parts_ref.at[source, j], dst_ref=parts_ref.at[source, j],
            send_sem=part_send.at[d - 1, j], recv_sem=part_recv.at[d - 1, j],
            device_id=slab_peer(d), device_id_type=MESH).wait_recv()

    y_ids = lax.broadcasted_iota(jnp.int32, (ry, chunk), 0).astype(jnp.float32).astype(jnp.bfloat16)
    row_ids = lax.broadcasted_iota(jnp.int32, (rows, chunk), 0)

    for copy in loads[channels:channels + 3]:
        copy.wait()
    for j in range(chunks):
        at = pl.ds(j * chunk, chunk)
        pix = pix_ref[:, at]
        start = start_ref[:, at]
        px = pix // ry
        py = (pix - px * ry).astype(jnp.float32).astype(jnp.bfloat16)
        length = jnp.clip((start - slab) * depth + count_ref[:, at], 0, depth)
        length = jnp.where(slab >= start, length, 0)
        row = jnp.where(length > 0, (length - 1) * rx + px, -1)
        row_ref[:, at] = row
        hot = jnp.where(y_ids == py, jnp.ones((), jnp.bfloat16), jnp.zeros((), jnp.bfloat16))
        onehot_ref[:, at] = hot
        twice = jnp.concatenate([hot, hot], axis=0)
        mask = row_ids == row
        for c in range(4):
            block = pl.ds(c * rows, rows)
            u = jnp.dot(pair_ref[block, :], twice, preferred_element_type=jnp.float32)
            part = jnp.sum(jnp.where(mask, u, 0.0), axis=0, keepdims=True)
            if c == 3:
                part = jnp.where(row < 0, 1.0, part)
            parts_ref[slab, j, pl.ds(c, 1), :] = part
        for d in range(1, ns):
            part_copy(d, j).start()

    for copy, _, receives in halos:
        pl.when(receives)(copy.wait_recv)
    x_ids = lax.broadcasted_iota(jnp.int32, (rx, ry), 0)
    lane_ids = lax.broadcasted_iota(jnp.int32, (rx, ry), 1)
    first_x = tile == 0
    last_x = tile == nt - 1
    for c in range(channels):
        for z in range(depth):
            g = grid_ref[c, z]
            if z > 0:
                below = grid_ref[c, z - 1]
            else:
                below = jnp.where(slab > 0, zhalo_ref[0, c], g)
            if z < depth - 1:
                above = grid_ref[c, z + 1]
            else:
                above = jnp.where(slab < ns - 1, zhalo_ref[1, c], g)
            xl = jnp.broadcast_to(xhalo_ref[0, c, pl.ds(z, 1), :], (rx, ry))
            xh = jnp.broadcast_to(xhalo_ref[1, c, pl.ds(z, 1), :], (rx, ry))
            xl = jnp.where(first_x, g, xl)
            xh = jnp.where(last_x, g, xh)
            left = jnp.where(x_ids == 0, xl, pltpu.roll(g, 1, 0))
            right = jnp.where(x_ids == rx - 1, xh, pltpu.roll(g, rx - 1, 0))
            down = jnp.where(lane_ids == 0, g, pltpu.roll(g, 1, 1))
            up = jnp.where(lane_ids == ry - 1, g, pltpu.roll(g, ry - 1, 1))
            smooth = (g - below) + (g - above) + (g - left) + (g - right) + (g - down) + (g - up)
            grad_ref[c, z] = (2.0 * TV_WEIGHT) * smooth

    loads[channels + 3].wait()
    row_ids16 = row_ids.astype(jnp.float32).astype(jnp.bfloat16)
    for j in range(chunks):
        for d in range(1, ns):
            part_wait(d, j)
        at = pl.ds(j * chunk, chunk)
        front_c = jnp.zeros((3, chunk), jnp.float32)
        front_t = jnp.ones((1, chunk), jnp.float32)
        beyond = jnp.full((3, chunk), BACKGROUND, jnp.float32)
        for s in range(ns - 1):
            here = slab > s
            pc = parts_ref[s, j, pl.ds(0, 3), :]
            pt = parts_ref[s, j, pl.ds(3, 1), :]
            front_c = jnp.where(here, front_c + front_t * pc, front_c)
            front_t = jnp.where(here, front_t * pt, front_t)
        for s in range(ns - 1, 0, -1):
            here = slab < s
            pc = parts_ref[s, j, pl.ds(0, 3), :]
            pt = parts_ref[s, j, pl.ds(3, 1), :]
            beyond = jnp.where(here, pc + pt * beyond, beyond)
        pc = parts_ref[slab, j, pl.ds(0, 3), :]
        pt = parts_ref[slab, j, pl.ds(3, 1), :]
        rendered = front_c + front_t * (pc + pt * beyond)
        residual = RENDER_WEIGHT * (rendered - target_ref[:, at])
        color_cot = front_t * residual
        trans_cot = front_t * jnp.sum(residual * beyond, axis=0, keepdims=True)
        hot = onehot_ref[:, at]
        twice = jnp.concatenate([hot, hot], axis=1)
        mask = row_ids16 == row_ref[:, at].astype(jnp.float32).astype(jnp.bfloat16)
        none = jnp.zeros((), jnp.bfloat16)
        for c in range(4):
            cot = color_cot[c:c + 1] if c < 3 else trans_cot
            top = cot.astype(jnp.bfloat16)
            low = (cot - top.astype(jnp.float32)).astype(jnp.bfloat16)
            spread = jnp.concatenate(
                [jnp.where(mask, top, none), jnp.where(mask, low, none)], axis=1)
            u = lax.dot_general(
                spread, twice, (((1,), (1,)), ((), ())), preferred_element_type=jnp.float32)
            block = pl.ds(c * rows, rows)
            if j == 0:
                table_ref[block, :] = u
            else:
                table_ref[block, :] += u

    zero = jnp.zeros((rx, ry), jnp.float32)
    suffix = [zero, zero, zero]
    later = zero
    squares = zero
    for z in range(depth - 1, -1, -1):
        w = weight_ref[z]
        after = trans_ref[z]
        later = later + after * table_ref[pl.ds(3 * rows + z * rx, rx), :]
        dw = zero
        for c in range(3):
            suffix[c] = suffix[c] + table_ref[pl.ds(c * rows + z * rx, rx), :]
            col = sig_ref[c + 1, z]
            dw = dw + col * suffix[c]
            out = grad_ref[c + 1, z] + w * suffix[c] * (col * (1.0 - col))
            grad_ref[c + 1, z] = out
            squares = squares + out * out
        dtau = after * dw - later
        later = later + w * dw
        out = grad_ref[0, z] + dtau * (sig_ref[0, z] * span)
        grad_ref[0, z] = out
        squares = squares + out * out

    local = jnp.sum(squares)

    def norm_copy(phase, slot, peer):
        return pltpu.make_async_remote_copy(
            src_ref=nsend_ref.at[phase], dst_ref=nrecv_ref.at[slot],
            send_sem=norm_send.at[slot], recv_sem=norm_recv.at[slot],
            device_id=peer, device_id_type=MESH)

    value = jnp.full((1, 128), local, jnp.float32)
    copies = []
    base = 0
    for phase, peers in enumerate(phases):
        nsend_ref[phase] = value
        group = [norm_copy(phase, base + i, peer) for i, peer in enumerate(peers)]
        for copy in group:
            copy.start()
        for i, copy in enumerate(group):
            copy.wait_recv()
            value = value + nrecv_ref[base + i]
        base += len(group)
        copies += group
    limit = CLIP_RMS * math.sqrt(4.0 * total_depth * (rx * nt) * ry)
    scale_ref[...] = limit / jnp.maximum(jnp.sqrt(value), limit)
    for copy in loads[channels + 4:]:
        copy.wait()
    for copy in copies:
        copy.wait_send()
    for copy, sends, _ in halos:
        pl.when(sends)(copy.wait_send)
    for j in range(chunks):
        for d in range(1, ns):
            part_copy(d, j).wait_send()


def direct(ns, nt):
    return ns * nt <= DIRECT_LIMIT


def adam_kernel(
    grid_ref, first_ref, second_ref, grad_ref, scale_ref,
    grid_hbm, first_hbm, second_hbm, grid_out, first_out, second_out, sem,
):
    channels, depth, rx, ry = grid_ref.shape
    scale = jnp.broadcast_to(scale_ref[0:1, 0:1], (rx, ry))
    copies = []
    for c in range(channels):
        for z in range(depth):
            clipped = grad_ref[c, z] * scale
            first = BETA_ONE * first_ref[c, z] + (1.0 - BETA_ONE) * clipped
            second = BETA_TWO * second_ref[c, z] + (1.0 - BETA_TWO) * clipped * clipped
            first_out[c, z] = first
            second_out[c, z] = second
            first_hat = first * (1.0 / (1.0 - BETA_ONE**STEP))
            second_hat = second * (1.0 / (1.0 - BETA_TWO**STEP))
            grid_out[c, z] = grid_ref[c, z] - LEARN_RATE * first_hat / (
                jnp.sqrt(second_hat) + EPSILON)
        pairs = ((first_out, first_hbm), (second_out, second_hbm), (grid_out, grid_hbm))
        for i, (a, b) in enumerate(pairs):
            copy = pltpu.make_async_copy(a.at[c], b.at[c], sem.at[i, c])
            copy.start()
            copies.append(copy)
    for copy in copies:
        copy.wait()


def per_device(voxel_grid, first_moment, second_moment, pixel_index, start_slab, ray_count, target):
    ns = lax.axis_size("slab")
    nt = lax.axis_size("tile")
    channels, depth, rx, ry = voxel_grid.shape
    rays = pixel_index.shape[0]
    chunk = math.gcd(rays, CHUNK)
    chunks = rays // chunk
    rows = depth * rx
    messages = ns * nt - 1 if direct(ns, nt) else nt + ns - 2
    f32 = jnp.float32
    vmem = pl.BlockSpec(memory_space=pltpu.VMEM)
    hbm = pl.BlockSpec(memory_space=pltpu.HBM)
    cells = jax.ShapeDtypeStruct(voxel_grid.shape, f32)
    staged = pl.pallas_call(
        functools.partial(kernel, ns, nt, chunk),
        out_shape=(cells, cells, cells, cells, jax.ShapeDtypeStruct((1, 128), f32)),
        in_specs=[hbm] * 7,
        out_specs=(vmem,) * 5,
        scratch_shapes=[
            pltpu.VMEM((1, rays), jnp.int32),
            pltpu.VMEM((1, rays), jnp.int32),
            pltpu.VMEM((1, rays), jnp.int32),
            pltpu.VMEM(target.shape, f32),
            pltpu.VMEM((channels * rows, 2 * ry), jnp.bfloat16),
            pltpu.VMEM((depth, rx, ry), f32),
            pltpu.VMEM((depth, rx, ry), f32),
            pltpu.VMEM((channels, depth, rx, ry), f32),
            pltpu.VMEM((ry, rays), jnp.bfloat16),
            pltpu.VMEM((1, rays), jnp.int32),
            pltpu.VMEM((ns, chunks, 4, chunk), f32),
            pltpu.VMEM((channels * rows, ry), f32),
            pltpu.VMEM((2, channels, depth, ry), f32),
            pltpu.VMEM((2, channels, depth, ry), f32),
            pltpu.VMEM((2, channels, rx, ry), f32),
            pltpu.VMEM((2, 1, 128), f32),
            pltpu.VMEM((messages, 1, 128), f32),
            pltpu.SemaphoreType.DMA((ns - 1, chunks)),
            pltpu.SemaphoreType.DMA((ns - 1, chunks)),
            pltpu.SemaphoreType.DMA((4,)),
            pltpu.SemaphoreType.DMA((4,)),
            pltpu.SemaphoreType.DMA((messages,)),
            pltpu.SemaphoreType.DMA((messages,)),
            pltpu.SemaphoreType.DMA((channels + 6,)),
        ],
        compiler_params=pltpu.CompilerParams(
            collective_id=0, has_side_effects=True, vmem_limit_bytes=32 * 1024 * 1024
        ),
        name="render_step",
    )(*(pltpu.with_memory_space_constraint(a, pltpu.HBM) for a in (
        voxel_grid,
        first_moment,
        second_moment,
        pixel_index.reshape(1, rays),
        start_slab.reshape(1, rays),
        ray_count.reshape(1, rays),
        target,
    )))
    return pl.pallas_call(
        adam_kernel,
        out_shape=(cells, cells, cells),
        in_specs=[vmem] * 5,
        out_specs=(hbm, hbm, hbm),
        scratch_shapes=[
            pltpu.VMEM(voxel_grid.shape, f32),
            pltpu.VMEM(voxel_grid.shape, f32),
            pltpu.VMEM(voxel_grid.shape, f32),
            pltpu.SemaphoreType.DMA((3, channels)),
        ],
        compiler_params=pltpu.CompilerParams(vmem_limit_bytes=32 * 1024 * 1024),
        name="adam",
    )(*staged)


def solution(mesh):
    cells = P(None, "slab", "tile", None)
    return jax.shard_map(
        per_device,
        mesh=mesh,
        in_specs=(cells, cells, cells, P("tile"), P("tile"), P("tile"), P(None, "tile")),
        out_specs=(cells, cells, cells),
        check_vma=False,
    )
```

```python
import functools
import math

import jax
import jax.numpy as jnp
from jax import lax
from jax.experimental import pallas as pl
from jax.experimental.pallas import tpu as pltpu
from jax.sharding import PartitionSpec as P

STEP = 20
RENDER_WEIGHT = 1000.0
TV_WEIGHT = 0.05
BACKGROUND = 1.0
STEP_SPAN = 4.0
CLIP_RMS = 0.25
LEARN_RATE = 0.02
BETA_ONE = 0.9
BETA_TWO = 0.99
EPSILON = 1e-08
CHUNK = 512
DIRECT_LIMIT = 64
MESH = pl.DeviceIdType.MESH


def kernel(
    ns, nt, chunk,
    grid_hbm, first_hbm, second_hbm, pix_hbm, start_hbm, count_hbm, target_hbm,
    grid_ref, first_ref, second_ref, grad_ref, scale_ref,
    pix_ref, start_ref, count_ref, target_ref,
    pair_ref, trans_ref, weight_ref, sig_ref, onehot_ref, row_ref, parts_ref, table_ref,
    edge_ref, xhalo_ref, zhalo_ref, nsend_ref, nrecv_ref,
    part_send, part_recv, halo_send, halo_recv, norm_send, norm_recv, load_sem,
):
    channels, depth, rx, ry = grid_ref.shape
    rays = pix_ref.shape[1]
    chunks = rays // chunk
    total_depth = depth * ns
    span = STEP_SPAN / total_depth
    rows = depth * rx
    slab = lax.axis_index("slab")
    tile = lax.axis_index("tile")

    def slab_peer(d):
        return {"slab": lax.rem(slab + d, ns)}

    def tile_peer(d):
        return {"tile": lax.rem(tile + d, nt)}

    if direct(ns, nt):
        pair = {"tile": tile + 1 - 2 * lax.rem(tile, 2)}
        half = nt // 2
        others = [
            {"slab": lax.rem(slab + k // half, ns), "tile": lax.rem(tile + 2 * (k % half), nt)}
            for k in range(1, ns * half)
        ]
        phases = [[pair], others]
        greeted = [pair] + [{"slab": lax.rem(slab + k // nt, ns), "tile": lax.rem(tile + k % nt, nt)} for k in range(1, ns * nt)]
        greeted = greeted[1:]
    else:
        phases = [[tile_peer(d) for d in range(1, nt)], [slab_peer(d) for d in range(1, ns)]]
        greeted = phases[0] + phases[1]

    loads = [
        pltpu.make_async_copy(grid_hbm.at[c], grid_ref.at[c], load_sem.at[c])
        for c in range(channels)
    ]
    rest = (
        (pix_hbm, pix_ref), (start_hbm, start_ref), (count_hbm, count_ref),
        (target_hbm, target_ref), (first_hbm, first_ref), (second_hbm, second_ref),
    )
    loads += [
        pltpu.make_async_copy(a, b, load_sem.at[channels + i]) for i, (a, b) in enumerate(rest)
    ]
    for copy in loads:
        copy.start()

    barrier = pltpu.get_barrier_semaphore()
    for peer in greeted:
        pl.semaphore_signal(barrier, inc=1, device_id=peer, device_id_type=MESH)

    for c in range(channels):
        loads[c].wait()
    edge_ref[0] = grid_ref[:, :, rx - 1, :]
    edge_ref[1] = grid_ref[:, :, 0, :]

    total = jnp.zeros((rx, ry), jnp.float32)
    before = jnp.ones((rx, ry), jnp.float32)
    sums = [jnp.zeros((rx, ry), jnp.float32) for _ in range(3)]
    for z in range(depth):
        s = grid_ref[0, z]
        e = jnp.exp(-jnp.abs(s))
        tau = (jnp.maximum(s, 0.0) + jnp.log1p(e)) * span
        sig_ref[0, z] = jnp.where(s >= 0, 1.0, e) / (1.0 + e)
        total = total + tau
        after = jnp.exp(-total)
        w = before * (1.0 - jnp.exp(-tau))
        before = after
        trans_ref[z] = after
        weight_ref[z] = w
        for c in range(3):
            col = 1.0 / (1.0 + jnp.exp(-grid_ref[c + 1, z]))
            sig_ref[c + 1, z] = col
            sums[c] = sums[c] + w * col
            table_ref[pl.ds(c * rows + z * rx, rx), :] = sums[c]
        table_ref[pl.ds(3 * rows + z * rx, rx), :] = after
    full = table_ref[...]
    high = full.astype(jnp.bfloat16)
    pair_ref[:, :ry] = high
    pair_ref[:, ry:] = (full - high.astype(jnp.float32)).astype(jnp.bfloat16)

    pl.semaphore_wait(barrier, len(greeted))

    def halo_copy(src, dst, i, peer):
        return pltpu.make_async_remote_copy(
            src_ref=src, dst_ref=dst, send_sem=halo_send.at[i], recv_sem=halo_recv.at[i],
            device_id=peer, device_id_type=MESH)

    halos = [
        (halo_copy(grid_ref.at[:, depth - 1], zhalo_ref.at[0], 0, slab_peer(1)), slab < ns - 1, slab > 0),
        (halo_copy(grid_ref.at[:, 0], zhalo_ref.at[1], 1, slab_peer(ns - 1)), slab > 0, slab < ns - 1),
        (halo_copy(edge_ref.at[0], xhalo_ref.at[0], 2, tile_peer(1)), tile < nt - 1, tile > 0),
        (halo_copy(edge_ref.at[1], xhalo_ref.at[1], 3, tile_peer(nt - 1)), tile > 0, tile < nt - 1),
    ]
    for copy, sends, _ in halos:
        pl.when(sends)(copy.start)

    def part_copy(d, j):
        return pltpu.make_async_remote_copy(
            src_ref=parts_ref.at[slab, j], dst_ref=parts_ref.at[slab, j],
            send_sem=part_send.at[d - 1, j], recv_sem=part_recv.at[d - 1, j],
            device_id=slab_peer(d), device_id_type=MESH)

    def part_wait(d, j):
        source = lax.rem(slab + ns - d, ns)
        pltpu.make_async_remote_copy(
            src_ref=parts_ref.at[source, j], dst_ref=parts_ref.at[source, j],
            send_sem=part_send.at[d - 1, j], recv_sem=part_recv.at[d - 1, j],
            device_id=slab_peer(d), device_id_type=MESH).wait_recv()

    y_ids = lax.broadcasted_iota(jnp.int32, (ry, chunk), 0).astype(jnp.float32).astype(jnp.bfloat16)
    row_ids = lax.broadcasted_iota(jnp.int32, (rows, chunk), 0)

    for copy in loads[channels:channels + 3]:
        copy.wait()
    for j in range(chunks):
        at = pl.ds(j * chunk, chunk)
        pix = pix_ref[:, at]
        start = start_ref[:, at]
        px = pix // ry
        py = (pix - px * ry).astype(jnp.float32).astype(jnp.bfloat16)
        length = jnp.clip((start - slab) * depth + count_ref[:, at], 0, depth)
        length = jnp.where(slab >= start, length, 0)
        row = jnp.where(length > 0, (length - 1) * rx + px, -1)
        row_ref[:, at] = row
        hot = jnp.where(y_ids == py, jnp.ones((), jnp.bfloat16), jnp.zeros((), jnp.bfloat16))
        onehot_ref[:, at] = hot
        twice = jnp.concatenate([hot, hot], axis=0)
        mask = row_ids == row
        for c in range(4):
            block = pl.ds(c * rows, rows)
            u = jnp.dot(pair_ref[block, :], twice, preferred_element_type=jnp.float32)
            part = jnp.sum(jnp.where(mask, u, 0.0), axis=0, keepdims=True)
            if c == 3:
                part = jnp.where(row < 0, 1.0, part)
            parts_ref[slab, j, pl.ds(c, 1), :] = part
        for d in range(1, ns):
            part_copy(d, j).start()

    for copy, _, receives in halos:
        pl.when(receives)(copy.wait_recv)
    x_ids = lax.broadcasted_iota(jnp.int32, (rx, ry), 0)
    lane_ids = lax.broadcasted_iota(jnp.int32, (rx, ry), 1)
    first_x = tile == 0
    last_x = tile == nt - 1
    for c in range(channels):
        for z in range(depth):
            g = grid_ref[c, z]
            if z > 0:
                below = grid_ref[c, z - 1]
            else:
                below = jnp.where(slab > 0, zhalo_ref[0, c], g)
            if z < depth - 1:
                above = grid_ref[c, z + 1]
            else:
                above = jnp.where(slab < ns - 1, zhalo_ref[1, c], g)
            xl = jnp.broadcast_to(xhalo_ref[0, c, pl.ds(z, 1), :], (rx, ry))
            xh = jnp.broadcast_to(xhalo_ref[1, c, pl.ds(z, 1), :], (rx, ry))
            xl = jnp.where(first_x, g, xl)
            xh = jnp.where(last_x, g, xh)
            left = jnp.where(x_ids == 0, xl, pltpu.roll(g, 1, 0))
            right = jnp.where(x_ids == rx - 1, xh, pltpu.roll(g, rx - 1, 0))
            down = jnp.where(lane_ids == 0, g, pltpu.roll(g, 1, 1))
            up = jnp.where(lane_ids == ry - 1, g, pltpu.roll(g, ry - 1, 1))
            smooth = (g - below) + (g - above) + (g - left) + (g - right) + (g - down) + (g - up)
            grad_ref[c, z] = (2.0 * TV_WEIGHT) * smooth

    loads[channels + 3].wait()
    row_ids16 = row_ids.astype(jnp.float32).astype(jnp.bfloat16)
    for j in range(chunks):
        for d in range(1, ns):
            part_wait(d, j)
        at = pl.ds(j * chunk, chunk)
        front_c = jnp.zeros((3, chunk), jnp.float32)
        front_t = jnp.ones((1, chunk), jnp.float32)
        beyond = jnp.full((3, chunk), BACKGROUND, jnp.float32)
        for s in range(ns - 1):
            here = slab > s
            pc = parts_ref[s, j, pl.ds(0, 3), :]
            pt = parts_ref[s, j, pl.ds(3, 1), :]
            front_c = jnp.where(here, front_c + front_t * pc, front_c)
            front_t = jnp.where(here, front_t * pt, front_t)
        for s in range(ns - 1, 0, -1):
            here = slab < s
            pc = parts_ref[s, j, pl.ds(0, 3), :]
            pt = parts_ref[s, j, pl.ds(3, 1), :]
            beyond = jnp.where(here, pc + pt * beyond, beyond)
        pc = parts_ref[slab, j, pl.ds(0, 3), :]
        pt = parts_ref[slab, j, pl.ds(3, 1), :]
        rendered = front_c + front_t * (pc + pt * beyond)
        residual = RENDER_WEIGHT * (rendered - target_ref[:, at])
        color_cot = front_t * residual
        trans_cot = front_t * jnp.sum(residual * beyond, axis=0, keepdims=True)
        hot = onehot_ref[:, at]
        twice = jnp.concatenate([hot, hot], axis=1)
        mask = row_ids16 == row_ref[:, at].astype(jnp.float32).astype(jnp.bfloat16)
        none = jnp.zeros((), jnp.bfloat16)
        for c in range(4):
            cot = color_cot[c:c + 1] if c < 3 else trans_cot
            top = cot.astype(jnp.bfloat16)
            low = (cot - top.astype(jnp.float32)).astype(jnp.bfloat16)
            spread = jnp.concatenate(
                [jnp.where(mask, top, none), jnp.where(mask, low, none)], axis=1)
            u = lax.dot_general(
                spread, twice, (((1,), (1,)), ((), ())), preferred_element_type=jnp.float32)
            block = pl.ds(c * rows, rows)
            if j == 0:
                table_ref[block, :] = u
            else:
                table_ref[block, :] += u

    zero = jnp.zeros((rx, ry), jnp.float32)
    suffix = [zero, zero, zero]
    later = zero
    squares = zero
    for z in range(depth - 1, -1, -1):
        w = weight_ref[z]
        after = trans_ref[z]
        later = later + after * table_ref[pl.ds(3 * rows + z * rx, rx), :]
        dw = zero
        for c in range(3):
            suffix[c] = suffix[c] + table_ref[pl.ds(c * rows + z * rx, rx), :]
            col = sig_ref[c + 1, z]
            dw = dw + col * suffix[c]
            out = grad_ref[c + 1, z] + w * suffix[c] * (col * (1.0 - col))
            grad_ref[c + 1, z] = out
            squares = squares + out * out
        dtau = after * dw - later
        later = later + w * dw
        out = grad_ref[0, z] + dtau * (sig_ref[0, z] * span)
        grad_ref[0, z] = out
        squares = squares + out * out

    local = jnp.sum(squares)

    def norm_copy(phase, slot, peer):
        return pltpu.make_async_remote_copy(
            src_ref=nsend_ref.at[phase], dst_ref=nrecv_ref.at[slot],
            send_sem=norm_send.at[slot], recv_sem=norm_recv.at[slot],
            device_id=peer, device_id_type=MESH)

    value = jnp.full((1, 128), local, jnp.float32)
    copies = []
    base = 0
    for phase, peers in enumerate(phases):
        nsend_ref[phase] = value
        group = [norm_copy(phase, base + i, peer) for i, peer in enumerate(peers)]
        for copy in group:
            copy.start()
        for i, copy in enumerate(group):
            copy.wait_recv()
            value = value + nrecv_ref[base + i]
        base += len(group)
        copies += group
    limit = CLIP_RMS * math.sqrt(4.0 * total_depth * (rx * nt) * ry)
    scale_ref[...] = limit / jnp.maximum(jnp.sqrt(value), limit)
    for copy in loads[channels + 4:]:
        copy.wait()
    for copy in copies:
        copy.wait_send()
    for copy, sends, _ in halos:
        pl.when(sends)(copy.wait_send)
    for j in range(chunks):
        for d in range(1, ns):
            part_copy(d, j).wait_send()


def direct(ns, nt):
    return ns * nt <= DIRECT_LIMIT and nt % 2 == 0


def adam_kernel(
    grid_ref, first_ref, second_ref, grad_ref, scale_ref,
    grid_hbm, first_hbm, second_hbm, grid_out, first_out, second_out, sem,
):
    channels, depth, rx, ry = grid_ref.shape
    scale = jnp.broadcast_to(scale_ref[0:1, 0:1], (rx, ry))
    copies = []
    for c in range(channels):
        for z in range(depth):
            clipped = grad_ref[c, z] * scale
            first = BETA_ONE * first_ref[c, z] + (1.0 - BETA_ONE) * clipped
            second = BETA_TWO * second_ref[c, z] + (1.0 - BETA_TWO) * clipped * clipped
            first_out[c, z] = first
            second_out[c, z] = second
            first_hat = first * (1.0 / (1.0 - BETA_ONE**STEP))
            second_hat = second * (1.0 / (1.0 - BETA_TWO**STEP))
            grid_out[c, z] = grid_ref[c, z] - LEARN_RATE * first_hat / (
                jnp.sqrt(second_hat) + EPSILON)
        pairs = ((first_out, first_hbm), (second_out, second_hbm), (grid_out, grid_hbm))
        for i, (a, b) in enumerate(pairs):
            copy = pltpu.make_async_copy(a.at[c], b.at[c], sem.at[i, c])
            copy.start()
            copies.append(copy)
    for copy in copies:
        copy.wait()


def per_device(voxel_grid, first_moment, second_moment, pixel_index, start_slab, ray_count, target):
    ns = lax.axis_size("slab")
    nt = lax.axis_size("tile")
    channels, depth, rx, ry = voxel_grid.shape
    rays = pixel_index.shape[0]
    chunk = math.gcd(rays, CHUNK)
    chunks = rays // chunk
    rows = depth * rx
    messages = ns * nt // 2 if direct(ns, nt) else nt + ns - 2
    f32 = jnp.float32
    vmem = pl.BlockSpec(memory_space=pltpu.VMEM)
    hbm = pl.BlockSpec(memory_space=pltpu.HBM)
    cells = jax.ShapeDtypeStruct(voxel_grid.shape, f32)
    staged = pl.pallas_call(
        functools.partial(kernel, ns, nt, chunk),
        out_shape=(cells, cells, cells, cells, jax.ShapeDtypeStruct((1, 128), f32)),
        in_specs=[hbm] * 7,
        out_specs=(vmem,) * 5,
        scratch_shapes=[
            pltpu.VMEM((1, rays), jnp.int32),
            pltpu.VMEM((1, rays), jnp.int32),
            pltpu.VMEM((1, rays), jnp.int32),
            pltpu.VMEM(target.shape, f32),
            pltpu.VMEM((channels * rows, 2 * ry), jnp.bfloat16),
            pltpu.VMEM((depth, rx, ry), f32),
            pltpu.VMEM((depth, rx, ry), f32),
            pltpu.VMEM((channels, depth, rx, ry), f32),
            pltpu.VMEM((ry, rays), jnp.bfloat16),
            pltpu.VMEM((1, rays), jnp.int32),
            pltpu.VMEM((ns, chunks, 4, chunk), f32),
            pltpu.VMEM((channels * rows, ry), f32),
            pltpu.VMEM((2, channels, depth, ry), f32),
            pltpu.VMEM((2, channels, depth, ry), f32),
            pltpu.VMEM((2, channels, rx, ry), f32),
            pltpu.VMEM((2, 1, 128), f32),
            pltpu.VMEM((messages, 1, 128), f32),
            pltpu.SemaphoreType.DMA((ns - 1, chunks)),
            pltpu.SemaphoreType.DMA((ns - 1, chunks)),
            pltpu.SemaphoreType.DMA((4,)),
            pltpu.SemaphoreType.DMA((4,)),
            pltpu.SemaphoreType.DMA((messages,)),
            pltpu.SemaphoreType.DMA((messages,)),
            pltpu.SemaphoreType.DMA((channels + 6,)),
        ],
        compiler_params=pltpu.CompilerParams(
            collective_id=0, has_side_effects=True, vmem_limit_bytes=32 * 1024 * 1024
        ),
        name="render_step",
    )(*(pltpu.with_memory_space_constraint(a, pltpu.HBM) for a in (
        voxel_grid,
        first_moment,
        second_moment,
        pixel_index.reshape(1, rays),
        start_slab.reshape(1, rays),
        ray_count.reshape(1, rays),
        target,
    )))
    return pl.pallas_call(
        adam_kernel,
        out_shape=(cells, cells, cells),
        in_specs=[vmem] * 5,
        out_specs=(hbm, hbm, hbm),
        scratch_shapes=[
            pltpu.VMEM(voxel_grid.shape, f32),
            pltpu.VMEM(voxel_grid.shape, f32),
            pltpu.VMEM(voxel_grid.shape, f32),
            pltpu.SemaphoreType.DMA((3, channels)),
        ],
        compiler_params=pltpu.CompilerParams(vmem_limit_bytes=32 * 1024 * 1024),
        name="adam",
    )(*staged)


def solution(mesh):
    cells = P(None, "slab", "tile", None)
    return jax.shard_map(
        per_device,
        mesh=mesh,
        in_specs=(cells, cells, cells, P("tile"), P("tile"), P("tile"), P(None, "tile")),
        out_specs=(cells, cells, cells),
        check_vma=False,
    )
```
